32 devices in a mesh: gx: 4 (over y, core), gy: 8 (over z, x).
Axes of the slice: x: 2, y: 2, z: 4, core: 2. Of those that a mesh axis runs over, the one named last changes fastest.
Arguments:
- position: float32 [4, 8, 3, 4096], P('gx', 'gy'), may hold values from 0 to 8, as said below
- velocity: float32 [4, 8, 3, 4096], P('gx', 'gy'), may hold values from -6 to 6
- mass: float32 [4, 8, 1, 4096], P('gx', 'gy'), may hold values from 0.3 to 3
- pair_list: int32 [4, 8, 32, 27], P('gx', 'gy'), may hold values from 0 to 287, as said below
- hot_leaf: int32 [4, 8, 8], P('gx', 'gy'), may hold values from 0 to 32, as said below
Outputs:
- displacement: float32 [4, 8, 3, 4096], P('gx', 'gy')
- new_velocity: float32 [4, 8, 3, 4096], P('gx', 'gy')
The draws below stay inside these ranges and needn't reach their ends.
Inputs may be any that keep to these rules, and one draw needn't show every extreme that they name: `pair_list`: entry k of every list names a leaf of neighbourhood block k mod 9. `position`: component 0 of a particle of cell (i, j) lies in [i, i + 1), component 1 in [j, j + 1), component 2 in [0, 1). `hot_leaf`: the slots of a cell hold distinct leaf numbers first and the empty mark 32 after them; cell (i, j) and cell (i, (j + 4) mod 8) hold exactly 8 hot leaves together.
All inputs are finite; a program needn't handle non-finite values.
Results may differ from the reference program's by a relative error of at most 0.00023.
Values sent between devices are 32-bit elements; how exact they have to be, the bound alone decides.
A program may use at most 64 MiB of HBM per device.

```python
import math
import jax
import jax.numpy as jnp
from jax import lax

LEAF = 128
LEAF_DEV = 32
PAIRS = 27
HOT = 8
PART = 4096
NGX = 4
NGY = 8
N_GX = 4
N_GY = 8


def draw_position(key, part):
    shape = (N_GX, N_GY, 3, LEAF_DEV * LEAF)
    inside = jax.random.uniform(key, shape, jnp.float32)
    row_index = lax.broadcasted_iota(jnp.int32, shape, 0).astype(jnp.float32)
    column_index = lax.broadcasted_iota(jnp.int32, shape, 1).astype(jnp.float32)
    channel = lax.broadcasted_iota(jnp.int32, shape, 2)
    offset = jnp.where(channel == 0, row_index, 0.0) + jnp.where(channel == 1, column_index, 0.0)
    return inside + offset


def draw_pair_list(key, part):
    shape = (N_GX, N_GY, LEAF_DEV, PAIRS)
    chosen = jax.random.randint(key, shape, 0, LEAF_DEV, jnp.int32)
    block = lax.broadcasted_iota(jnp.int32, shape, 3) % 9
    return block * LEAF_DEV + chosen


def draw_hot_leaf(key, part):
    first_key = jax.random.fold_in(key, 11)
    second_key = jax.random.fold_in(key, 23)
    half = N_GY // 2
    lower = jax.random.randint(first_key, (N_GX, half), 0, HOT + 1, jnp.int32)
    counts = jnp.concatenate([lower, HOT - lower], axis=1)
    scores = jax.random.randint(second_key, (N_GX, N_GY, LEAF_DEV), 0, 1 << 20, jnp.int32)
    leaves = lax.broadcasted_iota(jnp.int32, (N_GX, N_GY, LEAF_DEV), 2)
    order = jnp.argsort(scores * LEAF_DEV + leaves, axis=-1).astype(jnp.int32)[:, :, :HOT]
    slots = lax.broadcasted_iota(jnp.int32, (N_GX, N_GY, HOT), 2)
    return jnp.where(slots < counts[:, :, None], order, LEAF_DEV).astype(jnp.int32)


def shard_levels(stream_key, dims, cuts, low, top_value):
    def one(dim, shards_of):
        draws = jax.random.uniform(jax.random.fold_in(jax.random.fold_in(stream_key, 6), dim), (shards_of,), jnp.float32, low / len(cuts), top_value / len(cuts))
        return jnp.repeat(jnp.exp(draws), dims[dim] // shards_of).reshape((-1,) + (1,) * (len(dims) - dim - 1))

    level = one(*cuts[0])
    for cut in cuts[1:]:
        level = level * one(*cut)
    return level


def normal_values(rng, shape, scale, limit, shards=(), kind=jnp.bfloat16):
    array = scale * jax.random.normal(rng, shape, jnp.float32)
    if shards:
        array = array * shard_levels(rng, shape, shards, -0.22, 0.18)
    return jnp.clip(array, -limit, limit).astype(kind)


def setup_inputs(seed: int = 0) -> dict:
    keys = jax.random.split(jax.random.key(seed), 6)
    return {
        "position": draw_position(jax.random.fold_in(keys[5], 71), 0),
        "velocity": normal_values(keys[1], (NGX, NGY, 3, PART), 1.0, 6.0, ((0, 4), (1, 8)), jnp.float32),
        "mass": jnp.clip(jnp.exp(math.log(3.0) - 2.3025851 * jax.random.uniform(keys[2], (NGX, NGY, 1, PART), jnp.float32) ** shard_levels(keys[2], (NGX, NGY, 1, PART), ((0, 4), (1, 8)), -0.2, 0.2)), 0.3, 3.0),
        "pair_list": draw_pair_list(jax.random.fold_in(keys[5], 71), 0),
        "hot_leaf": draw_hot_leaf(jax.random.fold_in(keys[5], 71), 0),
    }


kernel_scale = 1.0
viscosity = 0.5
time_step = 0.5
base_entries = 9


def source_leaves(extended):
    channels = extended.shape[2]
    count = extended.shape[3] // LEAF
    return jnp.transpose(extended, (2, 0, 1, 3)).reshape(channels, 9 * count, LEAF)


def own_leaves(own):
    channels = own.shape[0]
    count = own.shape[1] // LEAF
    return jnp.transpose(own.reshape(channels, count, LEAF), (1, 0, 2))


def inverse_density(own, extended, pairs, usage):
    sources = source_leaves(extended)

    def one_leaf(inputs):
        target, chosen, used = inputs
        picked = jnp.take(sources, chosen, axis=1)
        near_mass = (picked[6] * used[:, None]).reshape(-1)
        near = picked.reshape(sources.shape[0], -1)
        diff = target[0:3, :, None] - near[0:3, None, :]
        weight = jnp.exp(-jnp.sum(diff * diff, axis=0) / kernel_scale)
        rho = target[6] + jnp.sum(near_mass[None, :] * weight, axis=1)
        return 1.0 / rho

    result = lax.map(one_leaf, (own_leaves(own), pairs, usage))
    return result.reshape(1, -1)


def acceleration(own, own_inverse, extended, extended_inverse, pairs, usage):
    sources = source_leaves(extended)
    source_inverse = source_leaves(extended_inverse)[0]
    targets = own_leaves(own)
    target_inverse = own_inverse.reshape(-1, LEAF)

    def one_leaf(inputs):
        target, target_q, chosen, used = inputs
        picked = jnp.take(sources, chosen, axis=1)
        near_mass = (picked[6] * used[:, None]).reshape(-1)
        near = picked.reshape(sources.shape[0], -1)
        near_q = jnp.take(source_inverse, chosen, axis=0).reshape(-1)
        diff = target[0:3, :, None] - near[0:3, None, :]
        weight = jnp.exp(-jnp.sum(diff * diff, axis=0) / kernel_scale)
        massed = near_mass[None, :] * weight
        press = massed * (2.0 / kernel_scale) * (target_q[:, None] + near_q[None, :])
        pushed = jnp.sum(press[None] * diff, axis=2)
        damped = jnp.sum((massed * near_q[None, :])[None] * (near[3:6, None, :] - target[3:6, :, None]), axis=2)
        return pushed + viscosity * damped

    result = lax.map(one_leaf, (targets, target_inverse, pairs, usage))
    return jnp.transpose(result, (1, 0, 2)).reshape(3, -1)


def neighbourhood(field):
    rows, columns = field.shape[0], field.shape[1]
    padded = jnp.pad(field, ((1, 1), (1, 1), (0, 0), (0, 0)))
    blocks = jnp.stack([jnp.stack([padded[a:a + rows, b:b + columns] for b in range(3)], axis=2) for a in range(3)], axis=2)
    return blocks.reshape((rows * columns, 3, 3) + field.shape[2:])


def entry_usage(flat_hot):
    leaves = jnp.arange(LEAF_DEV, dtype=jnp.int32)
    is_hot = jnp.any(flat_hot[:, :, None] == leaves[None, None, :], axis=1)
    entries = jnp.arange(PAIRS, dtype=jnp.int32)
    used = (entries[None, None, :] < base_entries) | is_hot[:, :, None]
    return jnp.where(used, 1.0, 0.0).astype(jnp.float32)


def section_all(position, velocity, mass, pair_list, hot_leaf):
    rows, columns = position.shape[0], position.shape[1]
    own = jnp.concatenate([position, velocity, mass], axis=2)
    flat_own = own.reshape((rows * columns,) + own.shape[2:])
    flat_pairs = pair_list.reshape((rows * columns,) + pair_list.shape[2:])
    usage = entry_usage(hot_leaf.reshape(rows * columns, -1))
    extended = neighbourhood(own)
    inverse = lax.map(lambda z: inverse_density(z[0], z[1], z[2], z[3]), (flat_own, extended, flat_pairs, usage))
    extended_inverse = neighbourhood(inverse.reshape(rows, columns, 1, -1))
    acc = lax.map(lambda z: acceleration(z[0], z[1], z[2], z[3], z[4], z[5]), (flat_own, inverse, extended, extended_inverse, flat_pairs, usage))
    return acc.reshape(position.shape)


def reference(position, velocity, mass, pair_list, hot_leaf):
    first = section_all(position, velocity, mass, pair_list, hot_leaf)
    mid_position = position + 0.5 * time_step * velocity
    mid_velocity = velocity + 0.5 * time_step * first
    second = section_all(mid_position, mid_velocity, mass, pair_list, hot_leaf)
    return time_step * mid_velocity, velocity + time_step * second
```

```python
import functools

import jax
import jax.numpy as jnp
from jax import lax
from jax.experimental import pallas as pl
from jax.experimental.pallas import tpu as pltpu
from jax.sharding import PartitionSpec as P

LEAF = 128
MESH = pl.DeviceIdType.MESH
BF16, F32 = jnp.bfloat16, jnp.float32

kernel_scale = 1.0
viscosity = 0.5
time_step = 0.5
base_entries = 9
COORD = (2.0 * 1.4426950408889634 / kernel_scale) ** 0.5
PUSH = 2.0 / (kernel_scale * COORD)
ABSENT = -1000.0

OWN, SIDES, CORNERS = (4,), (3, 5, 1, 7), (0, 2, 6, 8)


def rounded(value):
    return value.astype(BF16).astype(F32)


def loop(count, unroll, body):
    def several(i, carry):
        for u in range(unroll):
            body(i * unroll + u)
        return carry

    lax.fori_loop(0, count // unroll, several, 0)


def kernel(
    sizes, pos_ref, vel_ref, mass_ref, pair_ref, hot_ref, disp_ref, newv_ref,
    state, inverse, force, feature, push, target, weight_own, weight_far,
    partial, sums, rho_rows, mass_rows, mid, send_sem, recv_sem,
):
    count_x, count_y, leaves, listed, slots = sizes
    extra = listed // base_entries - 1
    tiles = leaves // 2
    gx, gy = lax.axis_index("gx"), lax.axis_index("gy")

    def inside(a, b):
        terms = []
        if a != 1:
            terms.append(gx > 0 if a == 0 else gx < count_x - 1)
        if b != 1:
            terms.append(gy > 0 if b == 0 else gy < count_y - 1)
        return terms[0] if len(terms) == 1 else terms[0] & terms[1]

    def device(a, b):
        return (jnp.clip(gx + a - 1, 0, count_x - 1), jnp.clip(gy + b - 1, 0, count_y - 1))

    def sent(buffer, number, block):
        a, b = divmod(block, 3)
        to = (1, 2 - b) if a == 1 else (2 - a, 1)
        source = 4 if a == 1 or b == 1 else 3 + b
        descriptor = pltpu.make_async_remote_copy(
            src_ref=buffer.at[source],
            dst_ref=buffer.at[block],
            send_sem=send_sem.at[number, block],
            recv_sem=recv_sem.at[number, block],
            device_id=device(*to),
            device_id_type=MESH,
        )
        return descriptor, inside(*to) if a == 1 or b == 1 else inside(2 - a, b)

    def start(buffer, number, blocks):
        for block in blocks:
            descriptor, valid = sent(buffer, number, block)
            pl.when(valid)(descriptor.start)

    def arrive(buffer, number, blocks):
        for block in blocks:
            pl.when(inside(*divmod(block, 3)))(sent(buffer, number, block)[0].wait_recv)

    messages = (state.at[0], state.at[1], inverse, force)

    row = lax.broadcasted_iota(jnp.int32, (8, LEAF), 0)
    low = row < 4
    last = row % 4 == 3
    zeros8 = jnp.zeros((8, LEAF), F32)
    ones_rows = jnp.where(row < 3, 1.0, 0.0).astype(F32)

    sides_of = ((1, 0), (1, 2), (0, 1), (2, 1))
    barrier = pltpu.get_barrier_semaphore()
    for a, b in sides_of:

        @pl.when(inside(a, b))
        def _():
            pl.semaphore_signal(barrier, inc=1, device_id=device(a, b), device_id_type=MESH)

    def span(leaf):
        return pl.ds(pl.multiple_of(leaf * LEAF, LEAF), LEAF)

    three = lax.broadcasted_iota(jnp.int32, (3, LEAF), 0)
    centre = jnp.where(
        three == 0, gx.astype(F32) + 0.5, jnp.where(three == 1, gy.astype(F32) + 0.5, 0.5)
    )

    def own_state(i):
        parts = [[], []]
        for half in range(2):
            leaf = 2 * i + half
            m = mass_ref[0, 0, :, span(leaf)]
            a1 = COORD * (pos_ref[0, 0, :, span(leaf)] - centre)
            a2 = a1 + (COORD * 0.5 * time_step) * vel_ref[0, 0, :, span(leaf)]
            mass_rows[pl.ds(leaf, 1), :] = m
            logm = jnp.log2(m)
            for section, a in enumerate((a1, a2)):
                parts[section] += [a, logm - 0.5 * jnp.sum(a * a, axis=0, keepdims=True)]
        for section in range(2):
            state[section, 4, i] = jnp.concatenate(parts[section], axis=0)

    loop(tiles, 4, own_state)
    pl.semaphore_wait(barrier, sum(inside(a, b).astype(jnp.int32) for a, b in sides_of))
    for section in range(2):
        start(messages[section], section, SIDES)

    for block in SIDES + CORNERS:

        @pl.when(jnp.logical_not(inside(*divmod(block, 3))))
        def _():
            def fill(i):
                for section in range(2):
                    state[section, block, i] = jnp.where(last, ABSENT, 0.0)
                force[block, i] = zeros8

            loop(tiles, 4, fill)
            inverse[block] = jnp.zeros((leaves, LEAF), F32)

    def paired(tile):
        hi = rounded(tile)
        lo = tile - hi
        return jnp.where(low, hi, pltpu.roll(lo, 4, 0)), jnp.where(low, pltpu.roll(hi, 4, 0), lo)

    def shifted(tile, block):
        a, b = divmod(block, 3)
        for steps, offset in ((3, a - 1), (2, b - 1)):
            if offset:
                d = COORD * offset
                coordinate = row % 4 == 3 - steps
                tile = (
                    tile
                    + jnp.where(coordinate, d, 0.0)
                    - jnp.where(last, d * pltpu.roll(tile, steps, 0) + 0.5 * d * d, 0.0)
                )
        return tile

    def prepare(section, blocks):
        for block in blocks:

            def one(i):
                halves = paired(shifted(state[section, block, i], block))
                for half in range(2):
                    feature[section, block * leaves + 2 * i + half] = jnp.concatenate(
                        [halves[half], ones_rows], axis=0
                    ).astype(BF16)

            loop(tiles, 4, one)

    def prepare_target(section):
        def one(i):
            tile = state[section, 4, i]
            hi = rounded(tile)
            lo = tile - hi
            square = tile * tile
            for half in range(2):
                if half == 0:
                    h, l = jnp.where(low, hi, pltpu.roll(hi, 4, 0)), jnp.where(low, lo, pltpu.roll(lo, 4, 0))
                else:
                    h, l = jnp.where(low, pltpu.roll(hi, 4, 0), hi), jnp.where(low, pltpu.roll(lo, 4, 0), lo)
                mine = (row // 4 == half) & jnp.logical_not(last)
                c = -0.5 * jnp.sum(jnp.where(mine, square, 0.0), axis=0, keepdims=True)
                c1 = rounded(c)
                c2 = rounded(c - c1)
                c3 = c - c1 - c2
                crows = jnp.where(row == 0, c1, jnp.where(row == 1, c2, jnp.where(row == 2, c3, 0.0)))
                stack = jnp.concatenate(
                    [jnp.where(last, 1.0, h), crows, jnp.where(last, 0.0, l), zeros8]
                    + [jnp.zeros((LEAF - 32, LEAF), F32)],
                    axis=0,
                )
                target[section, 2 * i + half] = stack.T.astype(BF16)

        loop(tiles, 2, one)

    def source(leaf, entry, block):
        return block * leaves + pair_ref[0, 0, leaf, entry] % leaves

    def slot_leaf(slot):
        return jnp.minimum(hot_ref[0, 0, slot], leaves - 1)

    def weigh(section, leaf, blocks, offsets, store):
        near = jnp.concatenate(
            [
                feature[section, source(leaf, offset + block, block)]
                for offset in offsets
                for block in blocks
            ],
            axis=1,
        )
        exponent = jnp.dot(
            target[section, leaf][:, 0:32],
            jnp.concatenate([near, near], axis=0),
            preferred_element_type=F32,
        )
        weight = jnp.exp2(exponent)
        store(weight.astype(BF16))
        pieces = [weight[:, k * LEAF : (k + 1) * LEAF] for k in range(weight.shape[1] // LEAF)]
        return functools.reduce(jnp.add, pieces)

    def hot_offsets(e):
        return (base_entries * (1 + e),)

    def keep(ref, index):
        def store(value):
            ref[index] = value

        return store

    def density(section, group):
        first = group is OWN
        final = group is CORNERS
        store_own = weight_own.at[section]
        store_far = weight_far.at[section, 0 if group is SIDES else 1]

        def finish(index, value):
            if not first:
                value = value + partial[index]
            if final:
                rho_rows[pl.ds(index, 1), :] = jnp.sum(value.T, axis=0, keepdims=True)
            else:
                partial[index] = value

        def base(i):
            ref = store_own.at[i, :, 0:LEAF] if first else store_far.at[i]
            finish(i, weigh(section, i, group, (0,), keep(ref, ...)))

        loop(leaves, 8 if not first else 8, base)

        def hot(s):
            leaf = slot_leaf(s)
            if first:
                offsets = tuple(base_entries * (1 + e) for e in range(extra))
                value = weigh(section, leaf, group, offsets, keep(store_own.at[leaves + s], ...))
            else:
                value = functools.reduce(
                    jnp.add,
                    [
                        weigh(
                            section, leaf, group, (base_entries * (1 + e),),
                            keep(store_far.at[leaves + extra * s + e], ...),
                        )
                        for e in range(extra)
                    ],
                )
            finish(leaves + s, value)

        loop(slots, 4, hot)

    def inverse_density():
        total = mass_rows[...] + rho_rows[pl.ds(0, leaves), :]
        leaf = lax.broadcasted_iota(jnp.int32, (leaves, LEAF), 0)
        for s in range(slots):
            total = total + jnp.where(leaf == hot_ref[0, 0, s], rho_rows[pl.ds(leaves + s, 1), :], 0.0)
        return 1.0 / total

    def store_push(block, i, tile):
        halves = paired(tile)
        for half in range(2):
            push[block * leaves + 2 * i + half] = jnp.concatenate(
                [halves[half], zeros8], axis=0
            ).astype(BF16)

    def spread(rows, i, block):
        first = jnp.broadcast_to(rows[block, pl.ds(2 * i, 1), :], (8, LEAF))
        second = jnp.broadcast_to(rows[block, pl.ds(2 * i + 1, 1), :], (8, LEAF))
        return jnp.where(low, first, second)

    def drive(tile, velocity, q):
        return q * jnp.where(last, 1.0, viscosity * velocity - PUSH * tile)

    def prepare_push1(blocks):
        for block in blocks:

            def one(i):
                here = state[0, block, i]
                velocity = (state[1, block, i] - here) * (1.0 / (COORD * 0.5 * time_step))
                store_push(
                    block, i, drive(shifted(here, block), velocity, spread(inverse, i, block))
                )

            loop(tiles, 4, one)

    def prepare_push2(blocks):
        for block in blocks:
            a, b = divmod(block, 3)

            def one(i):
                tile = force[block, i]
                for steps, offset in ((5, a - 1), (6, b - 1)):
                    if offset:
                        tile = tile - jnp.where(
                            row % 4 == steps - 5,
                            (2.0 / kernel_scale) * offset * pltpu.roll(tile, steps, 0),
                            0.0,
                        )
                store_push(block, i, tile)

            loop(tiles, 4, one)

    def gather(section, leaf, blocks, offsets, weight):
        near = []
        for offset in offsets:
            for block in blocks:
                index = source(leaf, offset + block, block)
                near.append(jnp.concatenate([feature[section, index], push[index]], axis=0))
        return lax.dot_general(
            weight, jnp.concatenate(near, axis=1), (((1,), (1,)), ((), ())),
            preferred_element_type=F32,
        )

    def accumulate(section, group):
        first = group is OWN
        load_own = weight_own.at[section]
        load_far = weight_far.at[section, 0 if group is SIDES else 1]

        def finish(index, value):
            sums[index] = value if first else sums[index] + value

        def base(i):
            weight = load_own[i, :, 0:LEAF] if first else load_far[i]
            finish(i, gather(section, i, group, (0,), weight))

        loop(leaves, 8, base)

        def hot(s):
            leaf = slot_leaf(s)
            if first:
                offsets = tuple(base_entries * (1 + e) for e in range(extra))
                value = gather(section, leaf, group, offsets, load_own[leaves + s])
            else:
                value = functools.reduce(
                    jnp.add,
                    [
                        gather(
                            section, leaf, group, (base_entries * (1 + e),),
                            load_far[leaves + extra * s + e],
                        )
                        for e in range(extra)
                    ],
                )
            finish(leaves + s, value)

        loop(slots, 4, hot)

    def combined(index):
        rows = sums[index].T
        near, pressed = rows[0:8], rows[16:24]
        near = near + pltpu.roll(near, 4, 0)
        near = jnp.where(last, jnp.broadcast_to(rows[8:9], (8, LEAF)), near)
        pressed = pressed + pltpu.roll(pressed, 4, 0)
        return jnp.where(low, near, pressed)

    def collect():
        def hot(s):
            rho_hot[s] = combined(leaves + s)

        loop(slots, 4, hot)

    rho_hot = mid.at[1]

    def accelerations(section, use):
        collect()

        def one(leaf):
            total = combined(leaf)
            for s in range(slots):
                mine = (hot_ref[0, 0, s] == leaf).astype(F32)
                total = total + mine * rho_hot[s]
            use(leaf, total)

        loop(leaves, 4, one)

    def acceleration(section, leaf, total, q, velocity):
        i, half = leaf // 2, leaf % 2
        a = state[section, 4, i, pl.ds(4 * half, 3), :]
        sq = total[7:8]
        return (
            PUSH * (q * (a * total[3:4] - total[0:3]) + a * sq)
            + total[4:7]
            - viscosity * velocity * sq
        )

    prepare_target(0)
    prepare(0, OWN)
    density(0, OWN)
    arrive(messages[0], 0, (3, 5))
    start(messages[0], 0, CORNERS)
    prepare_target(1)
    arrive(messages[0], 0, (1, 7))
    prepare(0, SIDES)
    density(0, SIDES)
    arrive(messages[1], 1, (3, 5))
    start(messages[1], 1, CORNERS)
    prepare(1, OWN)
    arrive(messages[0], 0, CORNERS)
    prepare(0, CORNERS)
    density(0, CORNERS)
    inverse[4] = inverse_density()
    start(inverse, 2, SIDES)

    density(1, OWN)
    arrive(messages[1], 1, (1, 7))
    prepare(1, SIDES)
    density(1, SIDES)
    arrive(inverse, 2, (3, 5))
    start(inverse, 2, CORNERS)
    arrive(messages[1], 1, CORNERS)
    prepare(1, CORNERS)
    density(1, CORNERS)
    rho_rows[pl.ds(0, leaves), :] = inverse_density()

    prepare_push1(OWN)
    accumulate(0, OWN)
    arrive(inverse, 2, (1, 7))
    prepare_push1(SIDES)
    accumulate(0, SIDES)
    arrive(inverse, 2, CORNERS)
    prepare_push1(CORNERS)
    accumulate(0, CORNERS)

    def use1(leaf, total):
        velocity = vel_ref[0, 0, :, span(leaf)]
        q = inverse[4, pl.ds(leaf, 1), :]
        moved = velocity + 0.5 * time_step * acceleration(0, leaf, total, q, velocity)
        mid[0, leaf, 0:3] = moved
        disp_ref[0, 0, :, span(leaf)] = time_step * moved

    accelerations(0, use1)

    def own_force(i):
        parts = []
        for half in range(2):
            leaf = 2 * i + half
            q = rho_rows[pl.ds(leaf, 1), :]
            a = state[1, 4, i, pl.ds(4 * half, 3), :]
            parts += [q * (viscosity * mid[0, leaf, 0:3] - PUSH * a), q]
        force[4, i] = jnp.concatenate(parts, axis=0)

    loop(tiles, 4, own_force)
    start(force, 3, SIDES)
    prepare_push2(OWN)
    accumulate(1, OWN)
    arrive(force, 3, (3, 5))
    start(force, 3, CORNERS)
    arrive(force, 3, (1, 7))
    prepare_push2(SIDES)
    accumulate(1, SIDES)
    arrive(force, 3, CORNERS)
    prepare_push2(CORNERS)
    accumulate(1, CORNERS)

    def use2(leaf, total):
        q = rho_rows[pl.ds(leaf, 1), :]
        acc = acceleration(1, leaf, total, q, mid[0, leaf, 0:3])
        newv_ref[0, 0, :, span(leaf)] = vel_ref[0, 0, :, span(leaf)] + time_step * acc

    accelerations(1, use2)

    for number, buffer in enumerate(messages):
        for block in SIDES + CORNERS:
            descriptor, valid = sent(buffer, number, block)
            pl.when(valid)(descriptor.wait_send)


def local(position, velocity, mass, pair_list, hot_leaf):
    leaves, listed = pair_list.shape[2:]
    slots = hot_leaf.shape[2]
    extra = listed // base_entries - 1
    sizes = (lax.axis_size("gx"), lax.axis_size("gy"), leaves, listed, slots)
    vmem = pl.BlockSpec(memory_space=pltpu.VMEM)
    smem = pl.BlockSpec(memory_space=pltpu.SMEM)
    shape = jax.ShapeDtypeStruct(position.shape, F32)
    tiles = leaves // 2
    return pl.pallas_call(
        functools.partial(kernel, sizes),
        out_shape=[shape, shape],
        in_specs=[vmem] * 3 + [smem] * 2,
        out_specs=[vmem] * 2,
        scratch_shapes=[
            pltpu.VMEM((2, 9, tiles, 8, LEAF), F32),
            pltpu.VMEM((9, leaves, LEAF), F32),
            pltpu.VMEM((9, tiles, 8, LEAF), F32),
            pltpu.VMEM((2, 9 * leaves, 16, LEAF), BF16),
            pltpu.VMEM((9 * leaves, 16, LEAF), BF16),
            pltpu.VMEM((2, leaves, LEAF, LEAF), BF16),
            pltpu.VMEM((2, leaves + slots, LEAF, extra * LEAF), BF16),
            pltpu.VMEM((2, 2, leaves + extra * slots, LEAF, 4 * LEAF), BF16),
            pltpu.VMEM((leaves + slots, LEAF, LEAF), F32),
            pltpu.VMEM((leaves + slots, LEAF, 32), F32),
            pltpu.VMEM((leaves + slots, LEAF), F32),
            pltpu.VMEM((leaves, LEAF), F32),
            pltpu.VMEM((2, leaves, 8, LEAF), F32),
            pltpu.SemaphoreType.DMA((4, 9)),
            pltpu.SemaphoreType.DMA((4, 9)),
        ],
        compiler_params=pltpu.CompilerParams(
            collective_id=0, has_side_effects=True, vmem_limit_bytes=60 * 2**20
        ),
    )(position, velocity, mass, pair_list, hot_leaf)


def solution(mesh):
    return jax.shard_map(
        local,
        mesh=mesh,
        in_specs=(
            P("gx", "gy", None, None),
            P("gx", "gy", None, None),
            P("gx", "gy", None, None),
            P("gx", "gy", None, None),
            P("gx", "gy", None),
        ),
        out_specs=(P("gx", "gy", None, None), P("gx", "gy", None, None)),
        check_vma=False,
    )
```

```python
import functools

import jax
import jax.numpy as jnp
from jax import lax
from jax.experimental import pallas as pl
from jax.experimental.pallas import tpu as pltpu
from jax.sharding import PartitionSpec as P

LEAF = 128
MESH = pl.DeviceIdType.MESH
BF16, F32 = jnp.bfloat16, jnp.float32

kernel_scale = 1.0
viscosity = 0.5
time_step = 0.5
base_entries = 9
COORD = (2.0 * 1.4426950408889634 / kernel_scale) ** 0.5
PUSH = 2.0 / (kernel_scale * COORD)
ABSENT = -1000.0
CHANNELS = 24

OWN, SIDES, CORNERS = (4,), (3, 5, 1, 7), (0, 2, 6, 8)


def rounded(value):
    return value.astype(BF16).astype(F32)


def loop(count, unroll, body):
    def several(i, carry):
        for u in range(unroll):
            body(i * unroll + u)
        return carry

    lax.fori_loop(0, count // unroll, several, 0)


def kernel(
    sizes, pos_ref, vel_ref, mass_ref, pair_ref, hot_ref, disp_ref, newv_ref,
    state, inverse, force, feature, push, target, weight_own, weight_far,
    partial, sums, rho_rows, mid, send_sem, recv_sem,
):
    count_x, count_y, leaves, listed, slots = sizes
    extra = listed // base_entries - 1
    tiles = leaves // 2
    gx, gy = lax.axis_index("gx"), lax.axis_index("gy")

    def inside(a, b):
        terms = []
        if a != 1:
            terms.append(gx > 0 if a == 0 else gx < count_x - 1)
        if b != 1:
            terms.append(gy > 0 if b == 0 else gy < count_y - 1)
        return terms[0] if len(terms) == 1 else terms[0] & terms[1]

    def device(a, b):
        return (jnp.clip(gx + a - 1, 0, count_x - 1), jnp.clip(gy + b - 1, 0, count_y - 1))

    def sent(buffer, number, block):
        a, b = divmod(block, 3)
        to = (1, 2 - b) if a == 1 else (2 - a, 1)
        source = 4 if a == 1 or b == 1 else 3 + b
        descriptor = pltpu.make_async_remote_copy(
            src_ref=buffer.at[source],
            dst_ref=buffer.at[block],
            send_sem=send_sem.at[number, block],
            recv_sem=recv_sem.at[number, block],
            device_id=device(*to),
            device_id_type=MESH,
        )
        return descriptor, inside(*to) if a == 1 or b == 1 else inside(2 - a, b)

    def start(buffer, number, blocks):
        for block in blocks:
            descriptor, valid = sent(buffer, number, block)
            pl.when(valid)(descriptor.start)

    def arrive(buffer, number, blocks):
        for block in blocks:
            pl.when(inside(*divmod(block, 3)))(sent(buffer, number, block)[0].wait_recv)

    messages = (state.at[0], state.at[1], inverse, force)

    row = lax.broadcasted_iota(jnp.int32, (8, LEAF), 0)
    low = row < 4
    last = row % 4 == 3
    zeros8 = jnp.zeros((8, LEAF), F32)
    ones_rows = jnp.where(row < 3, 1.0, 0.0).astype(F32)

    sides_of = ((1, 0), (1, 2), (0, 1), (2, 1))
    barrier = pltpu.get_barrier_semaphore()
    for a, b in sides_of:

        @pl.when(inside(a, b))
        def _():
            pl.semaphore_signal(barrier, inc=1, device_id=device(a, b), device_id_type=MESH)

    def lanes(component, pitch=4, count=leaves):
        return pl.ds(component, count, stride=pitch)

    centre = (gx.astype(F32) + 0.5, gy.astype(F32) + 0.5, 0.5)

    def own_state():
        logm = jnp.log2(mass_ref[...])
        first = [COORD * (pos_ref[d] - centre[d]) for d in range(3)]
        second = [first[d] + (COORD * 0.5 * time_step) * vel_ref[d] for d in range(3)]
        for section, a in enumerate((first, second)):
            for d in range(3):
                state[section, 4, lanes(d), :] = a[d]
            state[section, 4, lanes(3), :] = logm - 0.5 * (a[0] * a[0] + a[1] * a[1] + a[2] * a[2])

    def tile_rows(i):
        return pl.ds(pl.multiple_of(8 * i, 8), 8)

    own_state()
    pl.semaphore_wait(barrier, sum(inside(a, b).astype(jnp.int32) for a, b in sides_of))
    for section in range(2):
        start(messages[section], section, SIDES)

    for block in SIDES + CORNERS:

        @pl.when(jnp.logical_not(inside(*divmod(block, 3))))
        def _():
            def fill(i):
                for section in range(2):
                    state[section, block, tile_rows(i), :] = jnp.where(last, ABSENT, 0.0)
                force[block, tile_rows(i), :] = zeros8

            loop(tiles, 4, fill)
            inverse[block] = jnp.zeros((leaves, LEAF), F32)

    def paired(tile):
        hi = rounded(tile)
        lo = tile - hi
        return jnp.where(low, hi, pltpu.roll(lo, 4, 0)), jnp.where(low, pltpu.roll(hi, 4, 0), lo)

    def shifted(tile, block):
        a, b = divmod(block, 3)
        for steps, offset in ((3, a - 1), (2, b - 1)):
            if offset:
                d = COORD * offset
                coordinate = row % 4 == 3 - steps
                tile = (
                    tile
                    + jnp.where(coordinate, d, 0.0)
                    - jnp.where(last, d * pltpu.roll(tile, steps, 0) + 0.5 * d * d, 0.0)
                )
        return tile

    def prepare(section, blocks):
        for block in blocks:

            def one(i):
                halves = paired(shifted(state[section, block, tile_rows(i), :], block))
                for half in range(2):
                    feature[section, block * leaves + 2 * i + half] = jnp.concatenate(
                        [halves[half], ones_rows], axis=0
                    ).astype(BF16)

            loop(tiles, 8, one)

    def prepare_target(section):
        def one(i):
            tile = state[section, 4, tile_rows(i), :]
            hi = rounded(tile)
            lo = tile - hi
            square = tile * tile
            for half in range(2):
                if half == 0:
                    h, l = jnp.where(low, hi, pltpu.roll(hi, 4, 0)), jnp.where(low, lo, pltpu.roll(lo, 4, 0))
                else:
                    h, l = jnp.where(low, pltpu.roll(hi, 4, 0), hi), jnp.where(low, pltpu.roll(lo, 4, 0), lo)
                mine = (row // 4 == half) & jnp.logical_not(last)
                c = -0.5 * jnp.sum(jnp.where(mine, square, 0.0), axis=0, keepdims=True)
                c1 = rounded(c)
                c2 = rounded(c - c1)
                c3 = c - c1 - c2
                crows = jnp.where(row == 0, c1, jnp.where(row == 1, c2, jnp.where(row == 2, c3, 0.0)))
                stack = jnp.concatenate(
                    [jnp.where(last, 1.0, h), crows, jnp.where(last, 0.0, l), zeros8]
                    + [jnp.zeros((LEAF - 32, LEAF), F32)],
                    axis=0,
                )
                target[section, 2 * i + half] = stack.T.astype(BF16)

        loop(tiles, 4, one)

    def source(leaf, entry):
        return pair_ref[0, entry, 0, leaf]

    def slot_leaf(slot):
        return jnp.minimum(hot_ref[0, 0, slot], leaves - 1)

    def weigh(section, leaf, blocks, offsets, store):
        near = jnp.concatenate(
            [
                feature[section, source(leaf, offset + block)]
                for offset in offsets
                for block in blocks
            ],
            axis=1,
        )
        exponent = jnp.dot(
            target[section, leaf][:, 0:32],
            jnp.concatenate([near, near], axis=0),
            preferred_element_type=F32,
        )
        weight = jnp.exp2(exponent)
        store(weight.astype(BF16))
        pieces = [weight[:, k * LEAF : (k + 1) * LEAF] for k in range(weight.shape[1] // LEAF)]
        return functools.reduce(jnp.add, pieces)

    def hot_offsets(e):
        return (base_entries * (1 + e),)

    def keep(ref, index):
        def store(value):
            ref[index] = value

        return store

    def density(section, group):
        first = group is OWN
        final = group is CORNERS
        store_own = weight_own.at[section]
        store_far = weight_far.at[section, 0 if group is SIDES else 1]

        def finish(index, value):
            if not first:
                value = value + partial[index]
            if final:
                rho_rows[pl.ds(index, 1), :] = jnp.sum(value.T, axis=0, keepdims=True)
            else:
                partial[index] = value

        def base(i):
            ref = store_own.at[i, :, 0:LEAF] if first else store_far.at[i]
            finish(i, weigh(section, i, group, (0,), keep(ref, ...)))

        loop(leaves, 16, base)

        def hot(s):
            leaf = slot_leaf(s)
            if first:
                offsets = tuple(base_entries * (1 + e) for e in range(extra))
                value = weigh(section, leaf, group, offsets, keep(store_own.at[leaves + s], ...))
            else:
                value = functools.reduce(
                    jnp.add,
                    [
                        weigh(
                            section, leaf, group, (base_entries * (1 + e),),
                            keep(store_far.at[leaves + extra * s + e], ...),
                        )
                        for e in range(extra)
                    ],
                )
            finish(leaves + s, value)

        loop(slots, 4, hot)

    def inverse_density():
        total = mass_ref[...] + rho_rows[pl.ds(0, leaves), :]
        leaf = lax.broadcasted_iota(jnp.int32, (leaves, LEAF), 0)
        for s in range(slots):
            total = total + jnp.where(leaf == hot_ref[0, 0, s], rho_rows[pl.ds(leaves + s, 1), :], 0.0)
        return 1.0 / total

    def store_push(block, i, tile):
        halves = paired(tile)
        for half in range(2):
            push[block * leaves + 2 * i + half] = jnp.concatenate(
                [halves[half], zeros8], axis=0
            ).astype(BF16)

    def spread(rows, i, block):
        first = jnp.broadcast_to(rows[block, pl.ds(2 * i, 1), :], (8, LEAF))
        second = jnp.broadcast_to(rows[block, pl.ds(2 * i + 1, 1), :], (8, LEAF))
        return jnp.where(low, first, second)

    def drive(tile, velocity, q):
        return q * jnp.where(last, 1.0, viscosity * velocity - PUSH * tile)

    def prepare_push1(blocks):
        for block in blocks:

            def one(i):
                here = state[0, block, tile_rows(i), :]
                velocity = (state[1, block, tile_rows(i), :] - here) * (1.0 / (COORD * 0.5 * time_step))
                store_push(
                    block, i, drive(shifted(here, block), velocity, spread(inverse, i, block))
                )

            loop(tiles, 4, one)

    def prepare_push2(blocks):
        for block in blocks:
            a, b = divmod(block, 3)

            def one(i):
                tile = force[block, tile_rows(i), :]
                for steps, offset in ((5, a - 1), (6, b - 1)):
                    if offset:
                        tile = tile - jnp.where(
                            row % 4 == steps - 5,
                            (2.0 / kernel_scale) * offset * pltpu.roll(tile, steps, 0),
                            0.0,
                        )
                store_push(block, i, tile)

            loop(tiles, 4, one)

    def gather(section, leaf, blocks, offsets, weight):
        near = []
        for offset in offsets:
            for block in blocks:
                index = source(leaf, offset + block)
                near.append(jnp.concatenate([feature[section, index], push[index]], axis=0))
        return lax.dot_general(
            jnp.concatenate(near, axis=1), weight, (((1,), (1,)), ((), ())),
            preferred_element_type=F32,
        )[0:CHANNELS]

    def accumulate(section, group):
        first = group is OWN
        load_own = weight_own.at[section]
        load_far = weight_far.at[section, 0 if group is SIDES else 1]

        def finish(index, value):
            rows = pl.ds(pl.multiple_of(CHANNELS * index, 8), CHANNELS)
            sums[rows, :] = value if first else sums[rows, :] + value

        def base(i):
            weight = load_own[i, :, 0:LEAF] if first else load_far[i]
            finish(i, gather(section, i, group, (0,), weight))

        loop(leaves, 16, base)

        def hot(s):
            leaf = slot_leaf(s)
            if first:
                offsets = tuple(base_entries * (1 + e) for e in range(extra))
                value = gather(section, leaf, group, offsets, load_own[leaves + s])
            else:
                value = functools.reduce(
                    jnp.add,
                    [
                        gather(
                            section, leaf, group, (base_entries * (1 + e),),
                            load_far[leaves + extra * s + e],
                        )
                        for e in range(extra)
                    ],
                )
            finish(leaves + s, value)

        loop(slots, 4, hot)

    def acceleration(section, q, velocity):
        leaf = lax.broadcasted_iota(jnp.int32, (leaves, LEAF), 0)
        mine = [leaf == hot_ref[0, 0, s] for s in range(slots)]

        def channel(*rows):
            both = functools.reduce(
                jnp.add, [sums[lanes(r, CHANNELS, leaves + slots), :] for r in rows]
            )
            total = both[0:leaves]
            for s in range(slots):
                total = total + jnp.where(mine[s], both[leaves + s : leaves + s + 1], 0.0)
            return total

        s1, sq = channel(8), channel(19, 23)
        result = []
        for d in range(3):
            a = state[section, 4, lanes(d), :]
            result.append(
                PUSH * (q * (a * s1 - channel(d, d + 4)) + a * sq)
                + channel(16 + d, 20 + d)
                - viscosity * velocity[d] * sq
            )
        return result

    prepare_target(0)
    prepare(0, OWN)
    density(0, OWN)
    arrive(messages[0], 0, (3, 5))
    start(messages[0], 0, CORNERS)
    prepare_target(1)
    arrive(messages[0], 0, (1, 7))
    prepare(0, SIDES)
    density(0, SIDES)
    arrive(messages[1], 1, (3, 5))
    start(messages[1], 1, CORNERS)
    prepare(1, OWN)
    arrive(messages[0], 0, CORNERS)
    prepare(0, CORNERS)
    density(0, CORNERS)
    inverse[4] = inverse_density()
    start(inverse, 2, SIDES)

    density(1, OWN)
    arrive(messages[1], 1, (1, 7))
    prepare(1, SIDES)
    density(1, SIDES)
    arrive(inverse, 2, (3, 5))
    start(inverse, 2, CORNERS)
    arrive(messages[1], 1, CORNERS)
    prepare(1, CORNERS)
    density(1, CORNERS)
    rho_rows[pl.ds(0, leaves), :] = inverse_density()

    prepare_push1(OWN)
    accumulate(0, OWN)
    arrive(inverse, 2, (1, 7))
    prepare_push1(SIDES)
    accumulate(0, SIDES)
    arrive(inverse, 2, CORNERS)
    prepare_push1(CORNERS)
    accumulate(0, CORNERS)

    velocity = [vel_ref[d] for d in range(3)]
    acc = acceleration(0, inverse[4], velocity)
    moved = [velocity[d] + 0.5 * time_step * acc[d] for d in range(3)]
    q = rho_rows[pl.ds(0, leaves), :]
    for d in range(3):
        force[4, lanes(d), :] = q * (viscosity * moved[d] - PUSH * state[1, 4, lanes(d), :])
        mid[d] = moved[d]
        disp_ref[d] = time_step * moved[d]
    force[4, lanes(3), :] = q
    start(force, 3, SIDES)
    prepare_push2(OWN)
    accumulate(1, OWN)
    arrive(force, 3, (3, 5))
    start(force, 3, CORNERS)
    arrive(force, 3, (1, 7))
    prepare_push2(SIDES)
    accumulate(1, SIDES)
    arrive(force, 3, CORNERS)
    prepare_push2(CORNERS)
    accumulate(1, CORNERS)

    acc = acceleration(1, rho_rows[pl.ds(0, leaves), :], [mid[d] for d in range(3)])
    for d in range(3):
        newv_ref[d] = vel_ref[d] + time_step * acc[d]

    for number, buffer in enumerate(messages):
        for block in SIDES + CORNERS:
            descriptor, valid = sent(buffer, number, block)
            pl.when(valid)(descriptor.wait_send)


def local(position, velocity, mass, pair_list, hot_leaf):
    leaves, listed = pair_list.shape[2:]
    slots = hot_leaf.shape[2]
    extra = listed // base_entries - 1
    sizes = (lax.axis_size("gx"), lax.axis_size("gy"), leaves, listed, slots)
    vmem = pl.BlockSpec(memory_space=pltpu.VMEM)
    smem = pl.BlockSpec(memory_space=pltpu.SMEM)
    shape = jax.ShapeDtypeStruct((3, leaves, LEAF), F32)
    outs = pl.pallas_call(
        functools.partial(kernel, sizes),
        out_shape=[shape, shape],
        in_specs=[vmem] * 3 + [smem] * 2,
        out_specs=[vmem] * 2,
        scratch_shapes=[
            pltpu.VMEM((2, 9, 4 * leaves, LEAF), F32),
            pltpu.VMEM((9, leaves, LEAF), F32),
            pltpu.VMEM((9, 4 * leaves, LEAF), F32),
            pltpu.VMEM((2, 9 * leaves, 16, LEAF), BF16),
            pltpu.VMEM((9 * leaves, 16, LEAF), BF16),
            pltpu.VMEM((2, leaves, LEAF, LEAF), BF16),
            pltpu.VMEM((2, leaves + slots, LEAF, extra * LEAF), BF16),
            pltpu.VMEM((2, 2, leaves + extra * slots, LEAF, 4 * LEAF), BF16),
            pltpu.VMEM((leaves + slots, LEAF, LEAF), F32),
            pltpu.VMEM(((leaves + slots) * CHANNELS, LEAF), F32),
            pltpu.VMEM((leaves + slots, LEAF), F32),
            pltpu.VMEM((3, leaves, LEAF), F32),
            pltpu.SemaphoreType.DMA((4, 9)),
            pltpu.SemaphoreType.DMA((4, 9)),
        ],
        compiler_params=pltpu.CompilerParams(
            collective_id=0, has_side_effects=True, vmem_limit_bytes=60 * 2**20
        ),
    )(
        position.reshape(3, leaves, LEAF),
        velocity.reshape(3, leaves, LEAF),
        mass.reshape(leaves, LEAF),
        jnp.transpose(pair_list, (0, 3, 1, 2)),
        hot_leaf,
    )
    return tuple(out.reshape(position.shape) for out in outs)


def solution(mesh):
    return jax.shard_map(
        local,
        mesh=mesh,
        in_specs=(
            P("gx", "gy", None, None),
            P("gx", "gy", None, None),
            P("gx", "gy", None, None),
            P("gx", "gy", None, None),
            P("gx", "gy", None),
        ),
        out_specs=(P("gx", "gy", None, None), P("gx", "gy", None, None)),
        check_vma=False,
    )
```

```python
import functools

import jax
import jax.numpy as jnp
from jax import lax
from jax.experimental import pallas as pl
from jax.experimental.pallas import tpu as pltpu
from jax.sharding import PartitionSpec as P

LEAF = 128
MESH = pl.DeviceIdType.MESH
BF16, F32 = jnp.bfloat16, jnp.float32

kernel_scale = 1.0
viscosity = 0.5
time_step = 0.5
base_entries = 9
COORD = (2.0 * 1.4426950408889634 / kernel_scale) ** 0.5
PUSH = 2.0 / (kernel_scale * COORD)
ABSENT = -1000.0
CHANNELS = 24

OWN, SIDES, CORNERS = (4,), (3, 5, 1, 7), (0, 2, 6, 8)


def rounded(value):
    return value.astype(BF16).astype(F32)


def loop(count, unroll, body):
    def several(i, carry):
        for u in range(unroll):
            body(i * unroll + u)
        return carry

    if count == unroll:
        several(0, 0)
    else:
        lax.fori_loop(0, count // unroll, several, 0)


def kernel(
    sizes, pos_in, vel_in, mass_in, pair_in, hot_in, moved_out, acc_out,
    pos_ref, vel_ref, mass_ref, pair_ref, hot_ref,
    state, inverse, force, feature, push, target, weight_own, weight_far,
    partial, sums, rho_rows, mid, acc_ref, load_sem, send_sem, recv_sem,
):
    count_x, count_y, leaves, listed, slots = sizes
    extra = listed // base_entries - 1
    tiles = leaves // 2
    gx, gy = lax.axis_index("gx"), lax.axis_index("gy")

    def inside(a, b):
        terms = []
        if a != 1:
            terms.append(gx > 0 if a == 0 else gx < count_x - 1)
        if b != 1:
            terms.append(gy > 0 if b == 0 else gy < count_y - 1)
        return terms[0] if len(terms) == 1 else terms[0] & terms[1]

    def device(a, b):
        return (jnp.clip(gx + a - 1, 0, count_x - 1), jnp.clip(gy + b - 1, 0, count_y - 1))

    rows4, half4 = 4 * leaves, 2 * leaves
    messages = (
        (state.at[0], 0, half4),
        (state.at[0], half4, half4),
        (state.at[1], 0, rows4),
        (inverse, 0, leaves),
        (force, 0, half4),
        (force, half4, half4),
    )

    def sent(number, block):
        buffer, first, count = messages[number]
        a, b = divmod(block, 3)
        to = (1, 2 - b) if a == 1 else (2 - a, 1)
        source = 4 if a == 1 or b == 1 else 3 + b
        descriptor = pltpu.make_async_remote_copy(
            src_ref=buffer.at[source, pl.ds(first, count)],
            dst_ref=buffer.at[block, pl.ds(first, count)],
            send_sem=send_sem.at[number, block],
            recv_sem=recv_sem.at[number, block],
            device_id=device(*to),
            device_id_type=MESH,
        )
        return descriptor, inside(*to) if a == 1 or b == 1 else inside(2 - a, b)

    def start(number, blocks):
        for block in blocks:
            descriptor, valid = sent(number, block)
            pl.when(valid)(descriptor.start)

    def arrive(number, blocks):
        for block in blocks:
            pl.when(inside(*divmod(block, 3)))(sent(number, block)[0].wait_recv)

    def relay(number):
        arrive(number, (3, 5))
        start(number, CORNERS)

    row = lax.broadcasted_iota(jnp.int32, (8, LEAF), 0)
    low = row < 4
    last = row % 4 == 3
    zeros8 = jnp.zeros((8, LEAF), F32)
    ones_rows = jnp.where(row < 3, 1.0, 0.0).astype(F32)

    sides_of = ((1, 0), (1, 2), (0, 1), (2, 1))
    barrier = pltpu.get_barrier_semaphore()
    for a, b in sides_of:

        @pl.when(inside(a, b))
        def _():
            pl.semaphore_signal(barrier, inc=1, device_id=device(a, b), device_id_type=MESH)

    loads = [
        pltpu.make_async_copy(source, target_ref, load_sem.at[k])
        for k, (source, target_ref) in enumerate(
            ((pos_in, pos_ref), (vel_in, vel_ref), (mass_in, mass_ref), (pair_in, pair_ref), (hot_in, hot_ref))
        )
    ]
    for load in loads:
        load.start()
    for load in loads:
        load.wait()

    def lanes(component, pitch=4, count=leaves):
        return pl.ds(component, count, stride=pitch)

    centre = (gx.astype(F32) + 0.5, gy.astype(F32) + 0.5, 0.5)

    def own_state():
        logm = jnp.log2(mass_ref[...])
        first = [COORD * (pos_ref[d] - centre[d]) for d in range(3)]
        second = [first[d] + (COORD * 0.5 * time_step) * vel_ref[d] for d in range(3)]
        for section, a in enumerate((first, second)):
            for d in range(3):
                state[section, 4, lanes(d), :] = a[d]
            state[section, 4, lanes(3), :] = logm - 0.5 * (a[0] * a[0] + a[1] * a[1] + a[2] * a[2])

    def tile_rows(i):
        return pl.ds(pl.multiple_of(8 * i, 8), 8)

    own_state()
    pl.semaphore_wait(barrier, sum(inside(a, b).astype(jnp.int32) for a, b in sides_of))
    for number in range(3):
        start(number, SIDES)

    for block in SIDES + CORNERS:

        @pl.when(jnp.logical_not(inside(*divmod(block, 3))))
        def _():
            def fill(i):
                for section in range(2):
                    state[section, block, tile_rows(i), :] = jnp.where(last, ABSENT, 0.0)
                force[block, tile_rows(i), :] = zeros8

            loop(tiles, 4, fill)
            inverse[block] = jnp.zeros((leaves, LEAF), F32)

    def paired(tile):
        hi = rounded(tile)
        lo = tile - hi
        return jnp.where(low, hi, pltpu.roll(lo, 4, 0)), jnp.where(low, pltpu.roll(hi, 4, 0), lo)

    def shifted(tile, block):
        a, b = divmod(block, 3)
        for steps, offset in ((3, a - 1), (2, b - 1)):
            if offset:
                d = COORD * offset
                coordinate = row % 4 == 3 - steps
                tile = (
                    tile
                    + jnp.where(coordinate, d, 0.0)
                    - jnp.where(last, d * pltpu.roll(tile, steps, 0) + 0.5 * d * d, 0.0)
                )
        return tile

    def prepare(section, blocks):
        for block in blocks:

            def one(i):
                halves = paired(shifted(state[section, block, tile_rows(i), :], block))
                for half in range(2):
                    feature[section, block * leaves + 2 * i + half] = jnp.concatenate(
                        [halves[half], ones_rows], axis=0
                    ).astype(BF16)

            loop(tiles, tiles, one)

    def prepare_target(section):
        def one(i):
            tile = state[section, 4, tile_rows(i), :]
            hi = rounded(tile)
            lo = tile - hi
            square = tile * tile
            for half in range(2):
                if half == 0:
                    h, l = jnp.where(low, hi, pltpu.roll(hi, 4, 0)), jnp.where(low, lo, pltpu.roll(lo, 4, 0))
                else:
                    h, l = jnp.where(low, pltpu.roll(hi, 4, 0), hi), jnp.where(low, pltpu.roll(lo, 4, 0), lo)
                mine = (row // 4 == half) & jnp.logical_not(last)
                c = -0.5 * jnp.sum(jnp.where(mine, square, 0.0), axis=0, keepdims=True)
                c1 = rounded(c)
                c2 = rounded(c - c1)
                c3 = c - c1 - c2
                crows = jnp.where(row == 0, c1, jnp.where(row == 1, c2, jnp.where(row == 2, c3, 0.0)))
                stack = jnp.concatenate(
                    [jnp.where(last, 1.0, h), crows, jnp.where(last, 0.0, l), zeros8]
                    + [jnp.zeros((LEAF - 32, LEAF), F32)],
                    axis=0,
                )
                target[section, 2 * i + half] = stack.T.astype(BF16)

        loop(tiles, 4, one)

    def source(leaf, entry):
        return pair_ref[0, entry, 0, leaf]

    def slot_leaf(slot):
        return jnp.minimum(hot_ref[0, 0, slot], leaves - 1)

    def weigh(section, leaf, blocks, offsets, store):
        near = jnp.concatenate(
            [
                feature[section, source(leaf, offset + block)]
                for offset in offsets
                for block in blocks
            ],
            axis=1,
        )
        exponent = jnp.dot(
            target[section, leaf][:, 0:32],
            jnp.concatenate([near, near], axis=0),
            preferred_element_type=F32,
        )
        weight = jnp.exp2(exponent)
        store(weight.astype(BF16))
        pieces = [weight[:, k * LEAF : (k + 1) * LEAF] for k in range(weight.shape[1] // LEAF)]
        return functools.reduce(jnp.add, pieces)

    def hot_offsets(e):
        return (base_entries * (1 + e),)

    def keep(ref, index):
        def store(value):
            ref[index] = value

        return store

    def density(section, group):
        first = group is OWN
        final = group is CORNERS
        store_own = weight_own.at[section]
        store_far = weight_far.at[section, 0 if group is SIDES else 1]

        def finish(index, value):
            if not first:
                value = value + partial[section, index]
            if final:
                rho_rows[pl.ds(index, 1), :] = jnp.sum(value.T, axis=0, keepdims=True)
            else:
                partial[section, index] = value

        def base(i):
            ref = store_own.at[i, :, 0:LEAF] if first else store_far.at[i]
            finish(i, weigh(section, i, group, (0,), keep(ref, ...)))

        loop(leaves, leaves, base)

        def hot(s):
            leaf = slot_leaf(s)
            if first:
                offsets = tuple(base_entries * (1 + e) for e in range(extra))
                value = weigh(section, leaf, group, offsets, keep(store_own.at[leaves + s], ...))
            else:
                value = functools.reduce(
                    jnp.add,
                    [
                        weigh(
                            section, leaf, group, (base_entries * (1 + e),),
                            keep(store_far.at[leaves + extra * s + e], ...),
                        )
                        for e in range(extra)
                    ],
                )
            finish(leaves + s, value)

        loop(slots, slots, hot)

    def inverse_density():
        total = mass_ref[...] + rho_rows[pl.ds(0, leaves), :]
        leaf = lax.broadcasted_iota(jnp.int32, (leaves, LEAF), 0)
        for s in range(slots):
            total = total + jnp.where(leaf == hot_ref[0, 0, s], rho_rows[pl.ds(leaves + s, 1), :], 0.0)
        return 1.0 / total

    def store_push(block, i, tile):
        halves = paired(tile)
        for half in range(2):
            push[block * leaves + 2 * i + half] = jnp.concatenate(
                [halves[half], zeros8], axis=0
            ).astype(BF16)

    def spread(rows, i, block):
        first = jnp.broadcast_to(rows[block, pl.ds(2 * i, 1), :], (8, LEAF))
        second = jnp.broadcast_to(rows[block, pl.ds(2 * i + 1, 1), :], (8, LEAF))
        return jnp.where(low, first, second)

    def drive(tile, velocity, q):
        return q * jnp.where(last, 1.0, viscosity * velocity - PUSH * tile)

    def prepare_push1(blocks):
        for block in blocks:

            def one(i):
                here = state[0, block, tile_rows(i), :]
                velocity = (state[1, block, tile_rows(i), :] - here) * (1.0 / (COORD * 0.5 * time_step))
                store_push(
                    block, i, drive(shifted(here, block), velocity, spread(inverse, i, block))
                )

            loop(tiles, tiles, one)

    def prepare_push2(blocks):
        for block in blocks:
            a, b = divmod(block, 3)

            def one(i):
                tile = force[block, tile_rows(i), :]
                for steps, offset in ((5, a - 1), (6, b - 1)):
                    if offset:
                        tile = tile - jnp.where(
                            row % 4 == steps - 5,
                            (2.0 / kernel_scale) * offset * pltpu.roll(tile, steps, 0),
                            0.0,
                        )
                store_push(block, i, tile)

            loop(tiles, tiles, one)

    def gather(section, leaf, blocks, offsets, weight):
        near = []
        for offset in offsets:
            for block in blocks:
                index = source(leaf, offset + block)
                near.append(jnp.concatenate([feature[section, index], push[index]], axis=0))
        return lax.dot_general(
            weight, jnp.concatenate(near, axis=1), (((1,), (1,)), ((), ())),
            preferred_element_type=F32,
        )

    def accumulate(section, group, hot_too=True, chosen=None):
        first = group is OWN
        final = group is CORNERS
        load_own = weight_own.at[section]
        load_far = weight_far.at[section, 0 if group is SIDES else 1]

        def finish(index, value):
            kept = partial.at[section, index, :, 0:32]
            if not first:
                value = value + kept[...]
            if final:
                sums[pl.ds(CHANNELS * index, CHANNELS), :] = value.T[0:CHANNELS]
            else:
                kept[...] = value

        def base(i):
            weight = load_own[i, :, 0:LEAF] if first else load_far[i]
            finish(i, gather(section, i, group, (0,), weight))

        for i in range(leaves) if chosen is None else chosen:
            base(i)

        def hot(s):
            leaf = slot_leaf(s)
            if first:
                offsets = tuple(base_entries * (1 + e) for e in range(extra))
                value = gather(section, leaf, group, offsets, load_own[leaves + s])
            else:
                value = functools.reduce(
                    jnp.add,
                    [
                        gather(
                            section, leaf, group, (base_entries * (1 + e),),
                            load_far[leaves + extra * s + e],
                        )
                        for e in range(extra)
                    ],
                )
            finish(leaves + s, value)

        if hot_too:
            loop(slots, slots, hot)

    def acceleration(section, first, count, q, velocity):
        leaf = first + lax.broadcasted_iota(jnp.int32, (count, LEAF), 0)
        mine = [leaf == hot_ref[0, 0, s] for s in range(slots)]

        def channel(*rows):
            total = functools.reduce(
                jnp.add, [sums[lanes(CHANNELS * first + r, CHANNELS, count), :] for r in rows]
            )
            hot = functools.reduce(
                jnp.add, [sums[lanes(CHANNELS * leaves + r, CHANNELS, slots), :] for r in rows]
            )
            for s in range(slots):
                total = total + jnp.where(mine[s], hot[s : s + 1], 0.0)
            return total

        s1, sq = channel(8), channel(19, 23)
        result = []
        for d in range(3):
            a = state[section, 4, lanes(4 * first + d, 4, count), :]
            result.append(
                PUSH * (q * (a * s1 - channel(d, d + 4)) + a * sq)
                + channel(16 + d, 20 + d)
                - viscosity * velocity[d] * sq
            )
        return result

    prepare_target(0)
    prepare(0, OWN)
    density(0, OWN)
    prepare_target(1)
    prepare(1, OWN)
    density(1, OWN)
    relay(0)
    relay(1)

    for number in (0, 1):
        arrive(number, (1, 7))
    prepare(0, SIDES)
    density(0, SIDES)
    for number in (0, 1):
        arrive(number, CORNERS)
    prepare(0, CORNERS)
    relay(2)
    density(0, CORNERS)
    inverse[4] = inverse_density()
    start(3, SIDES)

    arrive(2, (1, 7))
    prepare(1, SIDES)
    density(1, SIDES)
    relay(3)
    prepare_push1(OWN)
    accumulate(0, OWN)
    arrive(2, CORNERS)
    prepare(1, CORNERS)
    density(1, CORNERS)
    rho_rows[pl.ds(0, leaves), :] = inverse_density()

    arrive(3, (1, 7))
    prepare_push1(SIDES)
    accumulate(0, SIDES)
    arrive(3, CORNERS)
    prepare_push1(CORNERS)
    half = leaves // 2
    for part in range(2):
        first = part * half
        accumulate(0, CORNERS, part == 0, range(first, first + half))
        here = pl.ds(first, half)
        velocity = [vel_ref[d, here, :] for d in range(3)]
        acc = acceleration(0, first, half, inverse[4, here, :], velocity)
        q = rho_rows[here, :]
        for d in range(3):
            moved = velocity[d] + 0.5 * time_step * acc[d]
            mid[d, here, :] = moved
            rows = lanes(4 * first + d, 4, half)
            force[4, rows, :] = q * (viscosity * moved - PUSH * state[1, 4, rows, :])
        force[4, lanes(4 * first + 3, 4, half), :] = q
        start(4 + part, SIDES)
    stores = [pltpu.make_async_copy(mid, moved_out, load_sem.at[0])]
    stores[0].start()

    prepare_push2(OWN)
    accumulate(1, OWN)
    relay(4)
    relay(5)
    for number in (4, 5):
        arrive(number, (1, 7))
    prepare_push2(SIDES)
    accumulate(1, SIDES)
    for number in (4, 5):
        arrive(number, CORNERS)
    prepare_push2(CORNERS)
    accumulate(1, CORNERS)
    acc = acceleration(1, 0, leaves, rho_rows[pl.ds(0, leaves), :], [mid[d] for d in range(3)])
    for d in range(3):
        acc_ref[d] = acc[d]
    stores.append(pltpu.make_async_copy(acc_ref, acc_out, load_sem.at[1]))
    stores[1].start()

    for number in range(len(messages)):
        for block in SIDES + CORNERS:
            descriptor, valid = sent(number, block)
            pl.when(valid)(descriptor.wait_send)
    for store in stores:
        store.wait()


def local(position, velocity, mass, pair_list, hot_leaf):
    leaves, listed = pair_list.shape[2:]
    slots = hot_leaf.shape[2]
    extra = listed // base_entries - 1
    sizes = (lax.axis_size("gx"), lax.axis_size("gy"), leaves, listed, slots)
    anywhere = pl.BlockSpec(memory_space=pl.ANY)
    shape = jax.ShapeDtypeStruct((3, leaves, LEAF), F32)
    moved, acc = pl.pallas_call(
        functools.partial(kernel, sizes),
        out_shape=[shape, shape],
        in_specs=[anywhere] * 5,
        out_specs=[anywhere] * 2,
        scratch_shapes=[
            pltpu.VMEM((3, leaves, LEAF), F32),
            pltpu.VMEM((3, leaves, LEAF), F32),
            pltpu.VMEM((leaves, LEAF), F32),
            pltpu.SMEM((1, listed, 1, leaves), jnp.int32),
            pltpu.SMEM((1, 1, slots), jnp.int32),
            pltpu.VMEM((2, 9, 4 * leaves, LEAF), F32),
            pltpu.VMEM((9, leaves, LEAF), F32),
            pltpu.VMEM((9, 4 * leaves, LEAF), F32),
            pltpu.VMEM((2, 9 * leaves, 16, LEAF), BF16),
            pltpu.VMEM((9 * leaves, 16, LEAF), BF16),
            pltpu.VMEM((2, leaves, LEAF, LEAF), BF16),
            pltpu.VMEM((2, leaves + slots, LEAF, extra * LEAF), BF16),
            pltpu.VMEM((2, 2, leaves + extra * slots, LEAF, 4 * LEAF), BF16),
            pltpu.VMEM((2, leaves + slots, LEAF, LEAF), F32),
            pltpu.VMEM(((leaves + slots) * CHANNELS, LEAF), F32),
            pltpu.VMEM((leaves + slots, LEAF), F32),
            pltpu.VMEM((3, leaves, LEAF), F32),
            pltpu.VMEM((3, leaves, LEAF), F32),
            pltpu.SemaphoreType.DMA((5,)),
            pltpu.SemaphoreType.DMA((6, 9)),
            pltpu.SemaphoreType.DMA((6, 9)),
        ],
        compiler_params=pltpu.CompilerParams(
            collective_id=0, has_side_effects=True, vmem_limit_bytes=60 * 2**20
        ),
    )(
        position.reshape(3, leaves, LEAF),
        velocity.reshape(3, leaves, LEAF),
        mass.reshape(leaves, LEAF),
        jnp.transpose(pair_list, (0, 3, 1, 2)),
        hot_leaf,
    )
    return (
        (time_step * moved).reshape(position.shape),
        (velocity.reshape(3, leaves, LEAF) + time_step * acc).reshape(position.shape),
    )


def solution(mesh):
    return jax.shard_map(
        local,
        mesh=mesh,
        in_specs=(
            P("gx", "gy", None, None),
            P("gx", "gy", None, None),
            P("gx", "gy", None, None),
            P("gx", "gy", None, None),
            P("gx", "gy", None),
        ),
        out_specs=(P("gx", "gy", None, None), P("gx", "gy", None, None)),
        check_vma=False,
    )
```

```python
import functools

import jax
import jax.numpy as jnp
from jax import lax
from jax.experimental import pallas as pl
from jax.experimental.pallas import tpu as pltpu
from jax.sharding import PartitionSpec as P

LEAF = 128
MESH = pl.DeviceIdType.MESH
BF16, F32 = jnp.bfloat16, jnp.float32

kernel_scale = 1.0
viscosity = 0.5
time_step = 0.5
base_entries = 9
COORD = (2.0 * 1.4426950408889634 / kernel_scale) ** 0.5
PUSH = 2.0 / (kernel_scale * COORD)
ABSENT = -1000.0
CHANNELS = 24

OWN, SIDES, CORNERS = (4,), (3, 5, 1, 7), (0, 2, 6, 8)


def rounded(value):
    return value.astype(BF16).astype(F32)


def loop(count, unroll, body):
    def several(i, carry):
        for u in range(unroll):
            body(i * unroll + u)
        return carry

    if count == unroll:
        several(0, 0)
    else:
        lax.fori_loop(0, count // unroll, several, 0)


def kernel(
    sizes, pos_in, vel_in, mass_in, pair_in, hot_in, moved_out, acc_out,
    pos_ref, vel_ref, mass_ref, pair_ref, hot_ref,
    state, inverse, force, feature, push, target, weight_own, weight_far,
    partial, sums, rho_rows, mid, acc_ref, load_sem, send_sem, recv_sem,
):
    count_x, count_y, leaves, listed, slots = sizes
    extra = listed // base_entries - 1
    tiles = leaves // 2
    gx, gy = lax.axis_index("gx"), lax.axis_index("gy")

    def inside(a, b):
        terms = []
        if a != 1:
            terms.append(gx > 0 if a == 0 else gx < count_x - 1)
        if b != 1:
            terms.append(gy > 0 if b == 0 else gy < count_y - 1)
        return terms[0] if len(terms) == 1 else terms[0] & terms[1]

    def device(a, b):
        return (jnp.clip(gx + a - 1, 0, count_x - 1), jnp.clip(gy + b - 1, 0, count_y - 1))

    rows4, half4 = 4 * leaves, 2 * leaves
    messages = (
        (state.at[0], 0, half4),
        (state.at[0], half4, half4),
        (state.at[1], 0, rows4),
        (inverse, 0, leaves),
        (force, 0, half4),
        (force, half4, half4),
    )

    def sent(number, block):
        buffer, first, count = messages[number]
        a, b = divmod(block, 3)
        to = (1, 2 - b) if a == 1 else (2 - a, 1)
        source = 4 if a == 1 or b == 1 else 3 + b
        descriptor = pltpu.make_async_remote_copy(
            src_ref=buffer.at[source, pl.ds(first, count)],
            dst_ref=buffer.at[block, pl.ds(first, count)],
            send_sem=send_sem.at[number, block],
            recv_sem=recv_sem.at[number, block],
            device_id=device(*to),
            device_id_type=MESH,
        )
        return descriptor, inside(*to) if a == 1 or b == 1 else inside(2 - a, b)

    def start(number, blocks):
        for block in blocks:
            descriptor, valid = sent(number, block)
            pl.when(valid)(descriptor.start)

    def arrive(number, blocks):
        for block in blocks:
            pl.when(inside(*divmod(block, 3)))(sent(number, block)[0].wait_recv)

    def relay(number):
        arrive(number, (3, 5))
        start(number, CORNERS)

    row = lax.broadcasted_iota(jnp.int32, (8, LEAF), 0)
    low = row < 4
    last = row % 4 == 3
    zeros8 = jnp.zeros((8, LEAF), F32)
    ones_rows = jnp.where(row < 3, 1.0, 0.0).astype(F32)

    sides_of = ((1, 0), (1, 2), (0, 1), (2, 1))
    barrier = pltpu.get_barrier_semaphore()
    for a, b in sides_of:

        @pl.when(inside(a, b))
        def _():
            pl.semaphore_signal(barrier, inc=1, device_id=device(a, b), device_id_type=MESH)

    loads = [
        pltpu.make_async_copy(source, target_ref, load_sem.at[k])
        for k, (source, target_ref) in enumerate(
            ((pos_in, pos_ref), (vel_in, vel_ref), (mass_in, mass_ref), (pair_in, pair_ref), (hot_in, hot_ref))
        )
    ]
    for load in loads:
        load.start()
    for load in loads:
        load.wait()

    def lanes(component, pitch=4, count=leaves):
        return pl.ds(component, count, stride=pitch)

    centre = (gx.astype(F32) + 0.5, gy.astype(F32) + 0.5, 0.5)

    def own_state():
        logm = jnp.log2(mass_ref[...])
        first = [COORD * (pos_ref[d] - centre[d]) for d in range(3)]
        second = [first[d] + (COORD * 0.5 * time_step) * vel_ref[d] for d in range(3)]
        for section, a in enumerate((first, second)):
            for d in range(3):
                state[section, 4, lanes(d), :] = a[d]
            state[section, 4, lanes(3), :] = logm - 0.5 * (a[0] * a[0] + a[1] * a[1] + a[2] * a[2])

    def tile_rows(i):
        return pl.ds(pl.multiple_of(8 * i, 8), 8)

    own_state()
    pl.semaphore_wait(barrier, sum(inside(a, b).astype(jnp.int32) for a, b in sides_of))
    for number in range(3):
        start(number, SIDES)

    for block in SIDES + CORNERS:

        @pl.when(jnp.logical_not(inside(*divmod(block, 3))))
        def _():
            def fill(i):
                for section in range(2):
                    state[section, block, tile_rows(i), :] = jnp.where(last, ABSENT, 0.0)
                force[block, tile_rows(i), :] = zeros8

            loop(tiles, 4, fill)
            inverse[block] = jnp.zeros((leaves, LEAF), F32)

    def paired(tile):
        hi = rounded(tile)
        lo = tile - hi
        return jnp.where(low, hi, pltpu.roll(lo, 4, 0)), jnp.where(low, pltpu.roll(hi, 4, 0), lo)

    def shifted(tile, block):
        a, b = divmod(block, 3)
        for steps, offset in ((3, a - 1), (2, b - 1)):
            if offset:
                d = COORD * offset
                coordinate = row % 4 == 3 - steps
                tile = (
                    tile
                    + jnp.where(coordinate, d, 0.0)
                    - jnp.where(last, d * pltpu.roll(tile, steps, 0) + 0.5 * d * d, 0.0)
                )
        return tile

    def prepare(section, blocks):
        for block in blocks:

            def one(i):
                halves = paired(shifted(state[section, block, tile_rows(i), :], block))
                for half in range(2):
                    feature[section, block * leaves + 2 * i + half] = jnp.concatenate(
                        [halves[half], ones_rows], axis=0
                    ).astype(BF16)

            loop(tiles, tiles, one)

    def prepare_target(section):
        def one(i):
            tile = state[section, 4, tile_rows(i), :]
            hi = rounded(tile)
            lo = tile - hi
            square = tile * tile
            for half in range(2):
                if half == 0:
                    h, l = jnp.where(low, hi, pltpu.roll(hi, 4, 0)), jnp.where(low, lo, pltpu.roll(lo, 4, 0))
                else:
                    h, l = jnp.where(low, pltpu.roll(hi, 4, 0), hi), jnp.where(low, pltpu.roll(lo, 4, 0), lo)
                mine = (row // 4 == half) & jnp.logical_not(last)
                c = -0.5 * jnp.sum(jnp.where(mine, square, 0.0), axis=0, keepdims=True)
                c1 = rounded(c)
                c2 = rounded(c - c1)
                c3 = c - c1 - c2
                crows = jnp.where(row == 0, c1, jnp.where(row == 1, c2, jnp.where(row == 2, c3, 0.0)))
                stack = jnp.concatenate(
                    [jnp.where(last, 1.0, h), crows, jnp.where(last, 0.0, l), zeros8]
                    + [jnp.zeros((LEAF - 32, LEAF), F32)],
                    axis=0,
                )
                target[section, 2 * i + half] = stack.T.astype(BF16)

        loop(tiles, 4, one)

    def source(leaf, entry):
        return pair_ref[0, entry, 0, leaf]

    def slot_leaf(slot):
        return jnp.minimum(hot_ref[0, 0, slot], leaves - 1)

    def weigh(section, leaf, blocks, offsets, store):
        near = jnp.concatenate(
            [
                feature[section, source(leaf, offset + block)]
                for offset in offsets
                for block in blocks
            ],
            axis=1,
        )
        exponent = jnp.dot(
            target[section, leaf][:, 0:32],
            jnp.concatenate([near, near], axis=0),
            preferred_element_type=F32,
        )
        weight = jnp.exp2(exponent)
        store(weight.astype(BF16))
        pieces = [weight[:, k * LEAF : (k + 1) * LEAF] for k in range(weight.shape[1] // LEAF)]
        return functools.reduce(jnp.add, pieces)

    def hot_offsets(e):
        return (base_entries * (1 + e),)

    def keep(ref, index):
        def store(value):
            ref[index] = value

        return store

    def density(section, group):
        first = group is OWN
        final = group is CORNERS
        store_own = weight_own.at[section]
        store_far = weight_far.at[section, 0 if group is SIDES else 1]

        def finish(index, value):
            if not first:
                value = value + partial[section, index]
            if final:
                rho_rows[pl.ds(index, 1), :] = jnp.sum(value.T, axis=0, keepdims=True)
            else:
                partial[section, index] = value

        def base(i):
            ref = store_own.at[i, :, 0:LEAF] if first else store_far.at[i]
            finish(i, weigh(section, i, group, (0,), keep(ref, ...)))

        loop(leaves, leaves, base)

        def hot(s):
            leaf = slot_leaf(s)
            if first:
                offsets = tuple(base_entries * (1 + e) for e in range(extra))
                value = weigh(section, leaf, group, offsets, keep(store_own.at[leaves + s], ...))
            else:
                value = functools.reduce(
                    jnp.add,
                    [
                        weigh(
                            section, leaf, group, (base_entries * (1 + e),),
                            keep(store_far.at[leaves + extra * s + e], ...),
                        )
                        for e in range(extra)
                    ],
                )
            finish(leaves + s, value)

        loop(slots, slots, hot)

    def inverse_density():
        total = mass_ref[...] + rho_rows[pl.ds(0, leaves), :]
        leaf = lax.broadcasted_iota(jnp.int32, (leaves, LEAF), 0)
        for s in range(slots):
            total = total + jnp.where(leaf == hot_ref[0, 0, s], rho_rows[pl.ds(leaves + s, 1), :], 0.0)
        return 1.0 / total

    def store_push(block, i, tile):
        halves = paired(tile)
        for half in range(2):
            push[block * leaves + 2 * i + half] = jnp.concatenate(
                [halves[half], zeros8], axis=0
            ).astype(BF16)

    def spread(rows, i, block):
        first = jnp.broadcast_to(rows[block, pl.ds(2 * i, 1), :], (8, LEAF))
        second = jnp.broadcast_to(rows[block, pl.ds(2 * i + 1, 1), :], (8, LEAF))
        return jnp.where(low, first, second)

    def drive(tile, velocity, q):
        return q * jnp.where(last, 1.0, viscosity * velocity - PUSH * tile)

    def prepare_push1(blocks):
        for block in blocks:

            def one(i):
                here = state[0, block, tile_rows(i), :]
                velocity = (state[1, block, tile_rows(i), :] - here) * (1.0 / (COORD * 0.5 * time_step))
                store_push(
                    block, i, drive(shifted(here, block), velocity, spread(inverse, i, block))
                )

            loop(tiles, tiles, one)

    def prepare_push2(blocks):
        for block in blocks:
            a, b = divmod(block, 3)

            def one(i):
                tile = force[block, tile_rows(i), :]
                for steps, offset in ((5, a - 1), (6, b - 1)):
                    if offset:
                        tile = tile - jnp.where(
                            row % 4 == steps - 5,
                            (2.0 / kernel_scale) * offset * pltpu.roll(tile, steps, 0),
                            0.0,
                        )
                store_push(block, i, tile)

            loop(tiles, tiles, one)

    def gather(section, leaf, blocks, offsets, weight):
        near = []
        for offset in offsets:
            for block in blocks:
                index = source(leaf, offset + block)
                near.append(jnp.concatenate([feature[section, index], push[index]], axis=0))
        return lax.dot_general(
            weight, jnp.concatenate(near, axis=1), (((1,), (1,)), ((), ())),
            preferred_element_type=F32,
        )

    def accumulate(section, group, hot_too=True, chosen=None):
        first = group is OWN
        final = group is CORNERS
        load_own = weight_own.at[section]
        load_far = weight_far.at[section, 0 if group is SIDES else 1]

        def finish(index, value):
            kept = partial.at[section, index, :, 0:32]
            if not first:
                value = value + kept[...]
            if final:
                sums[pl.ds(CHANNELS * index, CHANNELS), :] = value.T[0:CHANNELS]
            else:
                kept[...] = value

        def base(i):
            weight = load_own[i, :, 0:LEAF] if first else load_far[i]
            finish(i, gather(section, i, group, (0,), weight))

        for i in range(leaves) if chosen is None else chosen:
            base(i)

        def hot(s):
            leaf = slot_leaf(s)
            if first:
                offsets = tuple(base_entries * (1 + e) for e in range(extra))
                value = gather(section, leaf, group, offsets, load_own[leaves + s])
            else:
                value = functools.reduce(
                    jnp.add,
                    [
                        gather(
                            section, leaf, group, (base_entries * (1 + e),),
                            load_far[leaves + extra * s + e],
                        )
                        for e in range(extra)
                    ],
                )
            finish(leaves + s, value)

        if hot_too:
            loop(slots, slots, hot)

    def acceleration(section, first, count, q, velocity):
        leaf = first + lax.broadcasted_iota(jnp.int32, (count, LEAF), 0)
        mine = [leaf == hot_ref[0, 0, s] for s in range(slots)]

        def channel(*rows):
            total = functools.reduce(
                jnp.add, [sums[lanes(CHANNELS * first + r, CHANNELS, count), :] for r in rows]
            )
            hot = functools.reduce(
                jnp.add, [sums[lanes(CHANNELS * leaves + r, CHANNELS, slots), :] for r in rows]
            )
            for s in range(slots):
                total = total + jnp.where(mine[s], hot[s : s + 1], 0.0)
            return total

        s1, sq = channel(8), channel(19, 23)
        result = []
        for d in range(3):
            a = state[section, 4, lanes(4 * first + d, 4, count), :]
            result.append(
                PUSH * (q * (a * s1 - channel(d, d + 4)) + a * sq)
                + channel(16 + d, 20 + d)
                - viscosity * velocity[d] * sq
            )
        return result

    prepare_target(0)
    prepare(0, OWN)
    density(0, OWN)
    prepare_target(1)
    prepare(1, OWN)
    density(1, OWN)
    relay(0)
    relay(1)

    for number in (0, 1):
        arrive(number, (1, 7))
    prepare(0, SIDES)
    density(0, SIDES)
    for number in (0, 1):
        arrive(number, CORNERS)
    prepare(0, CORNERS)
    relay(2)
    density(0, CORNERS)
    inverse[4] = inverse_density()
    start(3, SIDES)

    arrive(2, (1, 7))
    prepare(1, SIDES)
    density(1, SIDES)
    prepare_push1(OWN)
    accumulate(0, OWN)
    arrive(2, CORNERS)
    prepare(1, CORNERS)
    relay(3)
    density(1, CORNERS)
    rho_rows[pl.ds(0, leaves), :] = inverse_density()

    arrive(3, (1, 7))
    prepare_push1(SIDES)
    accumulate(0, SIDES)
    arrive(3, CORNERS)
    prepare_push1(CORNERS)
    half = leaves // 2
    for part in range(2):
        first = part * half
        accumulate(0, CORNERS, part == 0, range(first, first + half))
        here = pl.ds(first, half)
        velocity = [vel_ref[d, here, :] for d in range(3)]
        acc = acceleration(0, first, half, inverse[4, here, :], velocity)
        q = rho_rows[here, :]
        for d in range(3):
            moved = velocity[d] + 0.5 * time_step * acc[d]
            mid[d, here, :] = moved
            rows = lanes(4 * first + d, 4, half)
            force[4, rows, :] = q * (viscosity * moved - PUSH * state[1, 4, rows, :])
        force[4, lanes(4 * first + 3, 4, half), :] = q
        start(4 + part, SIDES)
    stores = [pltpu.make_async_copy(mid, moved_out, load_sem.at[0])]
    stores[0].start()

    prepare_push2(OWN)
    accumulate(1, OWN)
    relay(4)
    relay(5)
    for number in (4, 5):
        arrive(number, (1, 7))
    prepare_push2(SIDES)
    accumulate(1, SIDES)
    for number in (4, 5):
        arrive(number, CORNERS)
    prepare_push2(CORNERS)
    accumulate(1, CORNERS)
    acc = acceleration(1, 0, leaves, rho_rows[pl.ds(0, leaves), :], [mid[d] for d in range(3)])
    for d in range(3):
        acc_ref[d] = acc[d]
    stores.append(pltpu.make_async_copy(acc_ref, acc_out, load_sem.at[1]))
    stores[1].start()

    for number in range(len(messages)):
        for block in SIDES + CORNERS:
            descriptor, valid = sent(number, block)
            pl.when(valid)(descriptor.wait_send)
    for store in stores:
        store.wait()


def local(position, velocity, mass, pair_list, hot_leaf):
    leaves, listed = pair_list.shape[2:]
    slots = hot_leaf.shape[2]
    extra = listed // base_entries - 1
    sizes = (lax.axis_size("gx"), lax.axis_size("gy"), leaves, listed, slots)
    anywhere = pl.BlockSpec(memory_space=pl.ANY)
    shape = jax.ShapeDtypeStruct((3, leaves, LEAF), F32)
    moved, acc = pl.pallas_call(
        functools.partial(kernel, sizes),
        out_shape=[shape, shape],
        in_specs=[anywhere] * 5,
        out_specs=[anywhere] * 2,
        scratch_shapes=[
            pltpu.VMEM((3, leaves, LEAF), F32),
            pltpu.VMEM((3, leaves, LEAF), F32),
            pltpu.VMEM((leaves, LEAF), F32),
            pltpu.SMEM((1, listed, 1, leaves), jnp.int32),
            pltpu.SMEM((1, 1, slots), jnp.int32),
            pltpu.VMEM((2, 9, 4 * leaves, LEAF), F32),
            pltpu.VMEM((9, leaves, LEAF), F32),
            pltpu.VMEM((9, 4 * leaves, LEAF), F32),
            pltpu.VMEM((2, 9 * leaves, 16, LEAF), BF16),
            pltpu.VMEM((9 * leaves, 16, LEAF), BF16),
            pltpu.VMEM((2, leaves, LEAF, LEAF), BF16),
            pltpu.VMEM((2, leaves + slots, LEAF, extra * LEAF), BF16),
            pltpu.VMEM((2, 2, leaves + extra * slots, LEAF, 4 * LEAF), BF16),
            pltpu.VMEM((2, leaves + slots, LEAF, LEAF), F32),
            pltpu.VMEM(((leaves + slots) * CHANNELS, LEAF), F32),
            pltpu.VMEM((leaves + slots, LEAF), F32),
            pltpu.VMEM((3, leaves, LEAF), F32),
            pltpu.VMEM((3, leaves, LEAF), F32),
            pltpu.SemaphoreType.DMA((5,)),
            pltpu.SemaphoreType.DMA((6, 9)),
            pltpu.SemaphoreType.DMA((6, 9)),
        ],
        compiler_params=pltpu.CompilerParams(
            collective_id=0, has_side_effects=True, vmem_limit_bytes=60 * 2**20
        ),
    )(
        position.reshape(3, leaves, LEAF),
        velocity.reshape(3, leaves, LEAF),
        mass.reshape(leaves, LEAF),
        jnp.transpose(pair_list, (0, 3, 1, 2)),
        hot_leaf,
    )
    return (
        (time_step * moved).reshape(position.shape),
        (velocity.reshape(3, leaves, LEAF) + time_step * acc).reshape(position.shape),
    )


def solution(mesh):
    return jax.shard_map(
        local,
        mesh=mesh,
        in_specs=(
            P("gx", "gy", None, None),
            P("gx", "gy", None, None),
            P("gx", "gy", None, None),
            P("gx", "gy", None, None),
            P("gx", "gy", None),
        ),
        out_specs=(P("gx", "gy", None, None), P("gx", "gy", None, None)),
        check_vma=False,
    )
```
